32 devices in a mesh: rows: 8 (over y, x, core), cols: 4 (over z).
Axes of the slice: x: 2, y: 2, z: 4, core: 2. Of those that a mesh axis runs over, the one named last changes fastest.
Arguments:
- surface_field: float32 [4096, 8192], P('rows', 'cols'), may hold values from -20 to 30
- land_words: int32 [4096, 256], P('rows', 'cols'), may hold values from -2147483648 to 2147483646
Outputs:
- level_one: float32 [2048, 4096], P('rows', 'cols')
- level_two: float32 [1024, 2048], P('rows', 'cols')
- level_three: float32 [512, 1024], P('rows', 'cols')
- level_four: float32 [256, 512], P('rows', 'cols')
- level_means: float32 [4], replicated
- level_maxima: float32 [4], replicated
The draws below stay inside these ranges and needn't reach their ends.
All inputs are finite; a program needn't handle non-finite values.
Results may differ from the reference program's by a relative error of at most 0.0001.
Values sent between devices are 32-bit elements; how exact they have to be, the bound alone decides.
A program may use at most 128 MiB of HBM per device.

```python
import math
import jax
import jax.numpy as jnp

NY = 4096
NX = 8192


def draw_surface_field(key, part):
    noise_key = jax.random.fold_in(jax.random.fold_in(key, 11), 0)
    rows_frac = jnp.arange(NY, dtype=jnp.float32) / NY
    cols_frac = jnp.arange(NX, dtype=jnp.float32) / NX
    trend = (1.0 + 2.0 * rows_frac)[:, None] * (1.0 + 2.0 * cols_frac)[None, :]
    noise = jnp.clip(jax.random.normal(noise_key, (NY, NX), jnp.float32), -6.0, 6.0)
    return (trend + noise).astype(jnp.float32)


def touch_ends(values, key, smallest, top_value):
    index_at = [jax.random.randint(jax.random.fold_in(key, axis), (), 0, length) for axis, length in enumerate(values.shape)]
    main_axis = values.shape.index(max(values.shape))
    next_to = index_at[:main_axis] + [(index_at[main_axis] + 1) % values.shape[main_axis]] + index_at[main_axis + 1:]
    return values.at[tuple(index_at)].set(smallest).at[tuple(next_to)].set(top_value)


def setup_inputs(seed: int = 0) -> dict:
    splits = jax.random.split(jax.random.key(seed), 3)
    surface_field = draw_surface_field(jax.random.fold_in(splits[2], 71), 0)
    land_words = touch_ends(jax.random.randint(splits[1], (NY, NX // 32), -2147483648, 2147483647), jax.random.fold_in(splits[1], 1), -2147483648, 2147483646).astype(jnp.int32)
    return dict(surface_field=surface_field, land_words=land_words)


stencil_weights = (0.125, 0.375, 0.375, 0.125)
floor_value = 0.05
mean_eps = 1e-6


def coarsen(extended):
    count_rows = (extended.shape[1] - 2) // 2
    count_cols = (extended.shape[2] - 2) // 2
    across = stencil_weights[0] * extended[:, :, 0:2 * count_cols:2]
    for offset in range(1, 4):
        across = across + stencil_weights[offset] * extended[:, :, offset:offset + 2 * count_cols:2]
    downward = stencil_weights[0] * across[:, 0:2 * count_rows:2, :]
    for offset in range(1, 4):
        downward = downward + stencil_weights[offset] * across[:, offset:offset + 2 * count_rows:2, :]
    return downward


def finish(partial_value):
    values = partial_value[0] / jnp.maximum(partial_value[1], floor_value)
    covers = partial_value[1]
    return values, covers, jnp.stack([covers * values, covers])


def reference(surface_field, land_words):
    expanded = jnp.repeat(land_words, 32, axis=1)
    shifts = jnp.arange(expanded.shape[1], dtype=jnp.int32) % 32
    land_flag = jnp.bitwise_and(jnp.right_shift(expanded, shifts[None, :]), 1)
    rows_index = jnp.arange(NY, dtype=jnp.int32).astype(jnp.float32)
    latitude = ((rows_index + 0.5) / NY - 0.5) * math.pi
    covers = land_flag.astype(jnp.float32) * jnp.cos(latitude)[:, None]
    stacked = jnp.stack([covers * surface_field, covers])
    outputs = []
    weighted = []
    totals = []
    maxima = []
    for level_step in range(4):
        wrapped = jnp.concatenate([stacked[:, :, -1:], stacked, stacked[:, :, :1]], axis=2)
        padded = jnp.pad(wrapped, ((0, 0), (1, 1), (0, 0)))
        values, covers, stacked = finish(coarsen(padded))
        outputs.append(values)
        weighted.append(jnp.sum(stacked[0]))
        totals.append(jnp.sum(covers))
        maxima.append(jnp.max(values))
    level_means = jnp.stack(weighted) / (jnp.stack(totals) + mean_eps)
    return outputs[0], outputs[1], outputs[2], outputs[3], level_means, jnp.stack(maxima)
```

```python
import functools
import math

import jax
import jax.numpy as jnp
from jax import lax
from jax.experimental import pallas as pl
from jax.experimental.pallas import tpu as pltpu
from jax.sharding import PartitionSpec as P

stencil_weights = (0.125, 0.375, 0.375, 0.125)
floor_value = 0.05
mean_eps = 1e-06
LEVELS = 4
LANES = 128
HALO = 16
MESH = pl.DeviceIdType.MESH


def kernel(
    row_devices,
    col_devices,
    field,
    land,
    level_one,
    level_two,
    level_three,
    level_four,
    means_ref,
    maxima_ref,
    fine,
    words,
    cosines,
    send_left,
    send_right,
    from_left,
    from_right,
    rows_top,
    rows_bottom,
    land_top,
    land_bottom,
    p0,
    c0,
    p1,
    c1,
    p2,
    c2,
    p3,
    c3,
    split,
    stat_own,
    stat_all,
    load_sem,
    halo_send,
    halo_recv,
    stat_send,
    stat_recv,
):
    rows, cols = field.shape
    tiles = cols // LANES
    count_words = land.shape[1]
    row_at = lax.axis_index("rows")
    col_at = lax.axis_index("cols")
    total_rows = rows * row_devices

    def device(down, right):
        return (
            lax.rem(row_at + down + row_devices, row_devices),
            lax.rem(col_at + right + col_devices, col_devices),
        )

    others = [
        (down, right)
        for down in range(row_devices)
        for right in range(col_devices)
        if (down, right) != (0, 0)
    ]

    def load(tile):
        start = tile * LANES
        if not isinstance(tile, int):
            start = pl.multiple_of(start, LANES)
        return pltpu.make_async_copy(
            field.at[:, pl.ds(start, LANES)], fine.at[tile], load_sem.at[tile]
        )

    load(0).start()
    load(tiles - 1).start()
    for tile in range(1, tiles - 1):
        load(tile).start()

    barrier = pltpu.get_barrier_semaphore()
    for down, right in others:
        pl.semaphore_signal(barrier, inc=1, device_id=device(down, right), device_id_type=MESH)

    own_words = land[...]
    if count_words < LANES:
        own_words = jnp.concatenate(
            [own_words, jnp.zeros((rows, LANES - count_words), jnp.int32)], axis=1
        )
    words[HALO : HALO + rows, :] = own_words
    lane = lax.broadcasted_iota(jnp.int32, (8, LANES), 1)

    def flags(tile, start, count):
        lanes = lax.broadcasted_iota(jnp.int32, (count, LANES), 1)
        place = tile * (LANES // 32) + lax.shift_right_logical(lanes, 5)
        word = jnp.take_along_axis(
            words[pl.ds(start, count), :], place, axis=1, mode="promise_in_bounds"
        )
        return jnp.bitwise_and(
            lax.shift_right_logical(word, jnp.bitwise_and(lanes, 31)), 1
        ).astype(jnp.float32)

    row_index = (
        row_at * rows - HALO + lax.broadcasted_iota(jnp.int32, (rows + 2 * HALO, LANES), 0)
    )
    latitude = ((row_index.astype(jnp.float32) + 0.5) / total_rows - 0.5) * math.pi
    on_globe = jnp.logical_and(row_index >= 0, row_index < total_rows)
    cosines[...] = jnp.where(on_globe, jnp.cos(latitude), 0.0)

    load(0).wait()
    send_left[0:HALO, :] = jnp.transpose(fine[0])[0:HALO, :]
    send_left[HALO:, :] = jnp.transpose(flags(0, HALO, rows))[0:HALO, :]
    load(tiles - 1).wait()
    send_right[0:HALO, :] = jnp.transpose(fine[tiles - 1])[LANES - HALO :, :]
    send_right[HALO:, :] = jnp.transpose(flags(tiles - 1, HALO, rows))[LANES - HALO :, :]

    zero_pad = ((p0, c0, 8), (p1, c1, 16), (p2, c2, 16), (p3, c3, 16))
    for product, cover, width in zero_pad:
        for ref in (product, cover):
            shape = (ref.shape[0], width, LANES)
            ref[:, 0:width, :] = jnp.zeros(shape, jnp.float32)
            ref[:, ref.shape[1] - width :, :] = jnp.zeros(shape, jnp.float32)

    pl.semaphore_wait(barrier, len(others))
    plan = (
        (field.at[rows - HALO : rows, :], rows_top, (1, 0)),
        (field.at[0:HALO, :], rows_bottom, (-1, 0)),
        (land.at[rows - HALO : rows, :], land_top, (1, 0)),
        (land.at[0:HALO, :], land_bottom, (-1, 0)),
        (send_left, from_right.at[:, LANES : LANES + rows], (0, -1)),
        (send_right, from_left.at[:, LANES : LANES + rows], (0, 1)),
        (send_left.at[:, 0:LANES], from_right.at[:, LANES + rows :], (-1, -1)),
        (send_right.at[:, 0:LANES], from_left.at[:, LANES + rows :], (-1, 1)),
        (send_left.at[:, rows - LANES :], from_right.at[:, 0:LANES], (1, -1)),
        (send_right.at[:, rows - LANES :], from_left.at[:, 0:LANES], (1, 1)),
    )
    copies = []
    for place, (source, target, (down, right)) in enumerate(plan):
        copy = pltpu.make_async_remote_copy(
            src_ref=source,
            dst_ref=target,
            send_sem=halo_send.at[place],
            recv_sem=halo_recv.at[place],
            device_id=device(down, right),
            device_id_type=MESH,
        )
        copy.start()
        copies.append(copy)

    def own_tile(tile):
        for start in range(0, rows, 64):
            cover = flags(tile, HALO + start, 64) * cosines[HALO + start : HALO + start + 64, :]
            c0[tile + 1, 24 + start : 88 + start, :] = cover
            p0[tile + 1, 24 + start : 88 + start, :] = cover * fine[tile, start : start + 64, :]

    own_tile(0)
    own_tile(tiles - 1)

    @pl.loop(1, tiles - 1)
    def _(tile):
        load(tile).wait()
        own_tile(tile)

    for copy in copies:
        copy.wait()

    for landed, at in ((land_top, 0), (land_bottom, HALO + rows)):
        halo_words = landed[...]
        if count_words < LANES:
            halo_words = jnp.concatenate(
                [halo_words, jnp.zeros((HALO, LANES - count_words), jnp.int32)], axis=1
            )
        words[at : at + HALO, :] = halo_words
    for landed, at in ((rows_top, 0), (rows_bottom, HALO + rows)):
        for tile in range(tiles):
            cover = flags(tile, at, HALO) * cosines[at : at + HALO, :]
            c0[tile + 1, 8 + at : 8 + at + HALO, :] = cover
            p0[tile + 1, 8 + at : 8 + at + HALO, :] = (
                cover * landed[:, tile * LANES : (tile + 1) * LANES]
            )
    filler = jnp.zeros((LANES - HALO, rows + 2 * LANES), jnp.float32)
    first = LANES - HALO
    last = LANES + rows + HALO
    for packet, tile, at_end in ((from_left, 0, True), (from_right, tiles + 1, False)):
        sides = []
        for part in (packet[0:HALO, :], packet[HALO:, :]):
            pieces = [filler, part] if at_end else [part, filler]
            sides.append(jnp.transpose(jnp.concatenate(pieces, axis=0))[first:last, :])
        cover = sides[1] * cosines[...]
        c0[tile, 8 : 8 + rows + 2 * HALO, :] = cover
        p0[tile, 8 : 8 + rows + 2 * HALO, :] = cover * sides[0]

    band_row = lax.broadcasted_iota(jnp.int32, (4 * LANES, LANES), 0)
    band_col = lax.broadcasted_iota(jnp.int32, (4 * LANES, LANES), 1)
    tap = band_row - (LANES - 1) - 2 * band_col
    band = jnp.where(
        jnp.logical_or(tap == 0, tap == 3),
        stencil_weights[0],
        jnp.where(jnp.logical_or(tap == 1, tap == 2), stencil_weights[1], 0.0),
    ).astype(jnp.bfloat16)

    stats = []
    sources = ((p0, c0), (p1, c1), (p2, c2), (p3, c3))
    outputs = (level_one, level_two, level_three, level_four)
    for level in range(LEVELS):
        product_in, cover_in = sources[level]
        output = outputs[level]
        own = output.shape[0]
        count = own + 16
        tiles_in = product_in.shape[0]
        tiles_out = output.shape[1] // LANES

        @pl.loop(0, tiles_in)
        def _(tile):
            offset = pl.multiple_of(tile * LANES, LANES)
            for place, ref in enumerate((product_in, cover_in)):
                taps = [ref[tile, pl.ds(7 + a, count, stride=2), :] for a in range(4)]
                down = stencil_weights[0] * (taps[0] + taps[3]) + stencil_weights[1] * (
                    taps[1] + taps[2]
                )
                high = down.astype(jnp.bfloat16)
                low = (down - high.astype(jnp.float32)).astype(jnp.bfloat16)
                at = 2 * place * count
                split[at : at + count, pl.ds(offset, LANES)] = high
                split[at + count : at + 2 * count, pl.ds(offset, LANES)] = low

        index = row_at * own - 8 + lax.broadcasted_iota(jnp.int32, (count, LANES), 0)
        inside = jnp.logical_and(index >= 0, index < own * row_devices)

        def across(start, width, table):
            result = jnp.dot(
                split[0 : 4 * count, pl.ds(start, width)],
                table,
                preferred_element_type=jnp.float32,
            )
            num = result[0:count] + result[count : 2 * count]
            den = result[2 * count : 3 * count] + result[3 * count :]
            value = num / jnp.maximum(den, floor_value)
            cover = jnp.where(inside, den, 0.0)
            return value, cover, cover * value

        def keep(tile, cover, product):
            if level + 1 < LEVELS:
                product_out, cover_out = sources[level + 1]
                product_out[tile, 16 : 16 + count, :] = product
                cover_out[tile, 16 : 16 + count, :] = cover

        if level + 1 < LEVELS:
            value, cover, product = across(0, 2 * LANES, band[2 * LANES :])
            keep(0, cover, product)
            value, cover, product = across((tiles_in - 2) * LANES, 2 * LANES, band[: 2 * LANES])
            keep(tiles_out + 1, cover, product)

        def own_columns(tile, carry):
            weighted, total, largest = carry
            value, cover, product = across(
                pl.multiple_of(tile * 2 * LANES, 2 * LANES), 4 * LANES, band
            )
            keep(tile + 1, cover, product)
            output[:, pl.ds(pl.multiple_of(tile * LANES, LANES), LANES)] = value[8 : 8 + own]

            def parts(array):
                return array[8 : 8 + own].reshape(own // 8, 8, LANES)

            return (
                weighted + jnp.sum(parts(product), axis=0),
                total + jnp.sum(parts(cover), axis=0),
                jnp.maximum(largest, jnp.max(parts(value), axis=0)),
            )

        zero = jnp.zeros((8, LANES), jnp.float32)
        start = (zero, zero, jnp.full((8, LANES), -jnp.inf, jnp.float32))
        stats.append(lax.fori_loop(0, tiles_out, own_columns, start))

    row = lax.broadcasted_iota(jnp.int32, (8, LANES), 0)
    gathered = []
    for kind, reduce in ((0, jnp.sum), (1, jnp.sum), (2, jnp.max)):
        tile = jnp.zeros((8, LANES), jnp.float32)
        for level in range(LEVELS):
            tile = jnp.where(row == level, reduce(stats[level][kind], axis=0, keepdims=True), tile)
        gathered.append(reduce(tile, axis=1, keepdims=True))
    stat_own[...] = jnp.where(
        lane == 0, gathered[0], jnp.where(lane == 1, gathered[1], gathered[2])
    )
    copies = []
    for place, (down, right) in enumerate(others):
        copy = pltpu.make_async_remote_copy(
            src_ref=stat_own,
            dst_ref=stat_all.at[place],
            send_sem=stat_send.at[place],
            recv_sem=stat_recv.at[place],
            device_id=device(down, right),
            device_id_type=MESH,
        )
        copy.start()
        copies.append(copy)
    for copy in copies:
        copy.wait()
    summed = stat_own[...] + jnp.sum(stat_all[...], axis=0)
    largest = jnp.maximum(stat_own[...], jnp.max(stat_all[...], axis=0))
    weighted = jnp.sum(jnp.where(lane == 0, summed, 0.0), axis=1, keepdims=True)
    total = jnp.sum(jnp.where(lane == 1, summed, 0.0), axis=1, keepdims=True)
    level_means = jnp.broadcast_to(weighted / (total + mean_eps), (8, LANES))
    for level in range(LEVELS):
        here = jnp.logical_and(row == level, lane == 2)
        means_ref[level] = jnp.sum(jnp.where(here, level_means, 0.0))
        maxima_ref[level] = jnp.sum(jnp.where(here, largest, 0.0))


def per_device(row_devices, col_devices, surface_field, land_words):
    rows, cols = surface_field.shape
    f32 = jnp.float32
    levels = tuple(
        jax.ShapeDtypeStruct((rows >> level, cols >> level), f32) for level in range(1, LEVELS + 1)
    )
    scratch = [
        pltpu.VMEM((cols // LANES, rows, LANES), f32),
        pltpu.VMEM((rows + 2 * HALO, LANES), jnp.int32),
        pltpu.VMEM((rows + 2 * HALO, LANES), f32),
        pltpu.VMEM((2 * HALO, rows), f32),
        pltpu.VMEM((2 * HALO, rows), f32),
        pltpu.VMEM((2 * HALO, rows + 2 * LANES), f32),
        pltpu.VMEM((2 * HALO, rows + 2 * LANES), f32),
        pltpu.VMEM((HALO, cols), f32),
        pltpu.VMEM((HALO, cols), f32),
        pltpu.VMEM((HALO, land_words.shape[1]), jnp.int32),
        pltpu.VMEM((HALO, land_words.shape[1]), jnp.int32),
    ]
    for level in range(LEVELS):
        shape = ((cols >> level) // LANES + 2, (rows >> level) + 48, LANES)
        scratch += [pltpu.VMEM(shape, f32)] * 2
    others = row_devices * col_devices - 1
    scratch += [
        pltpu.VMEM((4 * (rows // 2 + 16), cols + 2 * LANES), jnp.bfloat16),
        pltpu.VMEM((8, LANES), f32),
        pltpu.VMEM((others, 8, LANES), f32),
        pltpu.SemaphoreType.DMA((cols // LANES,)),
        pltpu.SemaphoreType.DMA((10,)),
        pltpu.SemaphoreType.DMA((10,)),
        pltpu.SemaphoreType.DMA((others,)),
        pltpu.SemaphoreType.DMA((others,)),
    ]
    vmem = pl.BlockSpec(memory_space=pltpu.VMEM)
    smem = pl.BlockSpec(memory_space=pltpu.SMEM)
    small = jax.ShapeDtypeStruct((LEVELS,), f32)
    return pl.pallas_call(
        functools.partial(kernel, row_devices, col_devices),
        out_shape=(*levels, small, small),
        in_specs=[pl.BlockSpec(memory_space=pl.ANY), vmem],
        out_specs=(vmem, vmem, vmem, vmem, smem, smem),
        scratch_shapes=scratch,
        compiler_params=pltpu.CompilerParams(
            collective_id=0, has_side_effects=True, vmem_limit_bytes=60 * 1024 * 1024
        ),
        name="coarsen_levels",
    )(surface_field, land_words)


def solution(mesh):
    return jax.shard_map(
        functools.partial(per_device, mesh.shape["rows"], mesh.shape["cols"]),
        mesh=mesh,
        in_specs=(P("rows", "cols"), P("rows", "cols")),
        out_specs=(
            P("rows", "cols"),
            P("rows", "cols"),
            P("rows", "cols"),
            P("rows", "cols"),
            P(),
            P(),
        ),
        check_vma=False,
    )
```

```python
import functools
import math

import jax
import jax.numpy as jnp
from jax import lax
from jax.experimental import pallas as pl
from jax.experimental.pallas import tpu as pltpu
from jax.sharding import PartitionSpec as P

stencil_weights = (0.125, 0.375, 0.375, 0.125)
floor_value = 0.05
mean_eps = 1e-06
LEVELS = 4
LANES = 128
HALO = 16
MESH = pl.DeviceIdType.MESH


def kernel(
    row_devices,
    col_devices,
    field,
    land,
    level_one,
    level_two,
    level_three,
    level_four,
    means_ref,
    maxima_ref,
    fine,
    words,
    cosines,
    send_left,
    send_right,
    from_left,
    from_right,
    rows_top,
    rows_bottom,
    land_top,
    land_bottom,
    p0,
    c0,
    p1,
    c1,
    p2,
    c2,
    p3,
    c3,
    split,
    stat_own,
    stat_both,
    stat_all,
    load_sem,
    halo_send,
    halo_recv,
    stat_send,
    stat_recv,
):
    rows, cols = field.shape
    tiles = cols // LANES
    count_words = land.shape[0]
    row_at = lax.axis_index("rows")
    col_at = lax.axis_index("cols")
    total_rows = rows * row_devices

    def device(down, right):
        return (
            lax.rem(row_at + down + row_devices, row_devices),
            lax.rem(col_at + right + col_devices, col_devices),
        )

    along_rows = [(down, 0) for down in range(1, row_devices)]
    along_cols = [(0, right) for right in range(1, col_devices)]
    corners = [(down, right) for down in (-1, 1) for right in (-1, 1)]
    partners = along_rows + along_cols + corners

    def load(tile):
        start = tile * LANES
        if not isinstance(tile, int):
            start = pl.multiple_of(start, LANES)
        return pltpu.make_async_copy(
            field.at[:, pl.ds(start, LANES)], fine.at[tile], load_sem.at[tile]
        )

    load(0).start()
    load(tiles - 1).start()
    for tile in range(1, tiles - 1):
        load(tile).start()

    barrier = pltpu.get_barrier_semaphore()
    for down, right in partners:
        pl.semaphore_signal(barrier, inc=1, device_id=device(down, right), device_id_type=MESH)

    def upright(array):
        if count_words < LANES:
            filler = jnp.zeros((LANES - count_words, array.shape[1]), jnp.int32)
            array = jnp.concatenate([array, filler], axis=0)
        return jnp.transpose(array)

    words[HALO : HALO + rows, :] = upright(land[...])
    lane = lax.broadcasted_iota(jnp.int32, (8, LANES), 1)

    def flags(tile, start, count):
        lanes = lax.broadcasted_iota(jnp.int32, (count, LANES), 1)
        place = tile * (LANES // 32) + lax.shift_right_logical(lanes, 5)
        word = jnp.take_along_axis(
            words[pl.ds(start, count), :], place, axis=1, mode="promise_in_bounds"
        )
        return jnp.bitwise_and(
            lax.shift_right_logical(word, jnp.bitwise_and(lanes, 31)), 1
        ).astype(jnp.float32)

    blocks = -(-(rows + 2 * HALO) // LANES)
    packed = (8 * (-(-blocks // 8)), LANES)
    row_index = (
        row_at * rows
        - HALO
        + lax.broadcasted_iota(jnp.int32, packed, 0) * LANES
        + lax.broadcasted_iota(jnp.int32, packed, 1)
    )
    latitude = ((row_index.astype(jnp.float32) + 0.5) / total_rows - 0.5) * math.pi
    on_globe = jnp.logical_and(row_index >= 0, row_index < total_rows)
    packed_cosines = jnp.where(on_globe, jnp.cos(latitude), 0.0)
    for block in range(blocks):
        size = min(LANES, rows + 2 * HALO - block * LANES)
        spread = jnp.broadcast_to(packed_cosines[block : block + 1, :], (LANES, LANES))
        cosines[block * LANES : block * LANES + size, :] = jnp.transpose(spread)[0:size, :]

    load(0).wait()
    send_left[0:HALO, :] = jnp.transpose(fine[0])[0:HALO, :]
    send_left[HALO:, :] = jnp.transpose(flags(0, HALO, rows))[0:HALO, :]
    load(tiles - 1).wait()
    send_right[0:HALO, :] = jnp.transpose(fine[tiles - 1])[LANES - HALO :, :]
    send_right[HALO:, :] = jnp.transpose(flags(tiles - 1, HALO, rows))[LANES - HALO :, :]

    zero_pad = ((p0, c0, 8), (p1, c1, 16), (p2, c2, 16), (p3, c3, 16))
    for product, cover, width in zero_pad:
        for ref in (product, cover):
            shape = (ref.shape[0], width, LANES)
            ref[:, 0:width, :] = jnp.zeros(shape, jnp.float32)
            ref[:, ref.shape[1] - width :, :] = jnp.zeros(shape, jnp.float32)

    pl.semaphore_wait(barrier, len(partners))
    plan = (
        (field.at[rows - HALO : rows, :], rows_top, (1, 0)),
        (field.at[0:HALO, :], rows_bottom, (-1, 0)),
        (land.at[:, rows - LANES : rows], land_top, (1, 0)),
        (land.at[:, 0:LANES], land_bottom, (-1, 0)),
        (send_left, from_right.at[:, LANES : LANES + rows], (0, -1)),
        (send_right, from_left.at[:, LANES : LANES + rows], (0, 1)),
        (send_left.at[:, 0:LANES], from_right.at[:, LANES + rows :], (-1, -1)),
        (send_right.at[:, 0:LANES], from_left.at[:, LANES + rows :], (-1, 1)),
        (send_left.at[:, rows - LANES :], from_right.at[:, 0:LANES], (1, -1)),
        (send_right.at[:, rows - LANES :], from_left.at[:, 0:LANES], (1, 1)),
    )
    copies = []
    for place, (source, target, (down, right)) in enumerate(plan):
        copy = pltpu.make_async_remote_copy(
            src_ref=source,
            dst_ref=target,
            send_sem=halo_send.at[place],
            recv_sem=halo_recv.at[place],
            device_id=device(down, right),
            device_id_type=MESH,
        )
        copy.start()
        copies.append(copy)

    def own_tile(tile):
        for start in range(0, rows, 64):
            cover = flags(tile, HALO + start, 64) * cosines[HALO + start : HALO + start + 64, :]
            c0[tile + 1, 24 + start : 88 + start, :] = cover
            p0[tile + 1, 24 + start : 88 + start, :] = cover * fine[tile, start : start + 64, :]

    own_tile(0)
    own_tile(tiles - 1)

    @pl.loop(1, tiles - 1)
    def _(tile):
        load(tile).wait()
        own_tile(tile)

    for copy in copies:
        copy.wait()

    words[0:HALO, :] = upright(land_top[...])[LANES - HALO :, :]
    words[HALO + rows :, :] = upright(land_bottom[...])[0:HALO, :]
    for landed, at in ((rows_top, 0), (rows_bottom, HALO + rows)):
        for tile in range(tiles):
            cover = flags(tile, at, HALO) * cosines[at : at + HALO, :]
            c0[tile + 1, 8 + at : 8 + at + HALO, :] = cover
            p0[tile + 1, 8 + at : 8 + at + HALO, :] = (
                cover * landed[:, tile * LANES : (tile + 1) * LANES]
            )
    filler = jnp.zeros((LANES - HALO, rows + 2 * LANES), jnp.float32)
    first = LANES - HALO
    last = LANES + rows + HALO
    for packet, tile, at_end in ((from_left, 0, True), (from_right, tiles + 1, False)):
        sides = []
        for part in (packet[0:HALO, :], packet[HALO:, :]):
            pieces = [filler, part] if at_end else [part, filler]
            sides.append(jnp.transpose(jnp.concatenate(pieces, axis=0))[first:last, :])
        cover = sides[1] * cosines[...]
        c0[tile, 8 : 8 + rows + 2 * HALO, :] = cover
        p0[tile, 8 : 8 + rows + 2 * HALO, :] = cover * sides[0]

    band_row = lax.broadcasted_iota(jnp.int32, (4 * LANES, LANES), 0)
    band_col = lax.broadcasted_iota(jnp.int32, (4 * LANES, LANES), 1)
    tap = band_row - (LANES - 1) - 2 * band_col
    band = jnp.where(
        jnp.logical_or(tap == 0, tap == 3),
        stencil_weights[0],
        jnp.where(jnp.logical_or(tap == 1, tap == 2), stencil_weights[1], 0.0),
    ).astype(jnp.bfloat16)

    stats = []
    sources = ((p0, c0), (p1, c1), (p2, c2), (p3, c3))
    outputs = (level_one, level_two, level_three, level_four)
    for level in range(LEVELS):
        product_in, cover_in = sources[level]
        output = outputs[level]
        own = output.shape[0]
        count = own + 16
        tiles_in = product_in.shape[0]
        tiles_out = output.shape[1] // LANES

        @pl.loop(0, tiles_in)
        def _(tile):
            offset = pl.multiple_of(tile * LANES, LANES)
            for place, ref in enumerate((product_in, cover_in)):
                taps = [ref[tile, pl.ds(7 + a, count, stride=2), :] for a in range(4)]
                down = stencil_weights[0] * (taps[0] + taps[3]) + stencil_weights[1] * (
                    taps[1] + taps[2]
                )
                high = down.astype(jnp.bfloat16)
                low = (down - high.astype(jnp.float32)).astype(jnp.bfloat16)
                at = 2 * place * count
                split[at : at + count, pl.ds(offset, LANES)] = high
                split[at + count : at + 2 * count, pl.ds(offset, LANES)] = low

        index = row_at * own - 8 + lax.broadcasted_iota(jnp.int32, (count, LANES), 0)
        inside = jnp.logical_and(index >= 0, index < own * row_devices)

        def across(start, width, table):
            result = jnp.dot(
                split[0 : 4 * count, pl.ds(start, width)],
                table,
                preferred_element_type=jnp.float32,
            )
            num = result[0:count] + result[count : 2 * count]
            den = result[2 * count : 3 * count] + result[3 * count :]
            value = num / jnp.maximum(den, floor_value)
            cover = jnp.where(inside, den, 0.0)
            return value, cover, cover * value

        def keep(tile, cover, product):
            if level + 1 < LEVELS:
                product_out, cover_out = sources[level + 1]
                product_out[tile, 16 : 16 + count, :] = product
                cover_out[tile, 16 : 16 + count, :] = cover

        if level + 1 < LEVELS:
            value, cover, product = across(0, 2 * LANES, band[2 * LANES :])
            keep(0, cover, product)
            value, cover, product = across((tiles_in - 2) * LANES, 2 * LANES, band[: 2 * LANES])
            keep(tiles_out + 1, cover, product)

        def own_columns(tile, carry):
            weighted, total, largest = carry
            value, cover, product = across(
                pl.multiple_of(tile * 2 * LANES, 2 * LANES), 4 * LANES, band
            )
            keep(tile + 1, cover, product)
            output[:, pl.ds(pl.multiple_of(tile * LANES, LANES), LANES)] = value[8 : 8 + own]

            def parts(array):
                return array[8 : 8 + own].reshape(own // 8, 8, LANES)

            return (
                weighted + jnp.sum(parts(product), axis=0),
                total + jnp.sum(parts(cover), axis=0),
                jnp.maximum(largest, jnp.max(parts(value), axis=0)),
            )

        zero = jnp.zeros((8, LANES), jnp.float32)
        start = (zero, zero, jnp.full((8, LANES), -jnp.inf, jnp.float32))
        stats.append(lax.fori_loop(0, tiles_out, own_columns, start))

    row = lax.broadcasted_iota(jnp.int32, (8, LANES), 0)
    gathered = []
    for kind, reduce in ((0, jnp.sum), (1, jnp.sum), (2, jnp.max)):
        tile = jnp.zeros((8, LANES), jnp.float32)
        for level in range(LEVELS):
            tile = jnp.where(row == level, reduce(stats[level][kind], axis=0, keepdims=True), tile)
        gathered.append(reduce(tile, axis=1, keepdims=True))
    stat_own[...] = jnp.where(
        lane == 0, gathered[0], jnp.where(lane == 1, gathered[1], gathered[2])
    )
    slot = 0
    source = stat_own
    for group in (along_rows, along_cols):
        copies = []
        for place, (down, right) in enumerate(group):
            copy = pltpu.make_async_remote_copy(
                src_ref=source,
                dst_ref=stat_all.at[slot + place],
                send_sem=stat_send.at[slot + place],
                recv_sem=stat_recv.at[slot + place],
                device_id=device(down, right),
                device_id_type=MESH,
            )
            copy.start()
            copies.append(copy)
        for copy in copies:
            copy.wait()
        arrived = stat_all[slot : slot + len(group)]
        summed = source[...] + jnp.sum(arrived, axis=0)
        largest = jnp.maximum(source[...], jnp.max(arrived, axis=0))
        stat_both[...] = jnp.where(lane < 2, summed, largest)
        slot += len(group)
        source = stat_both
    weighted = jnp.sum(jnp.where(lane == 0, summed, 0.0), axis=1, keepdims=True)
    total = jnp.sum(jnp.where(lane == 1, summed, 0.0), axis=1, keepdims=True)
    level_means = jnp.broadcast_to(weighted / (total + mean_eps), (8, LANES))
    for level in range(LEVELS):
        here = jnp.logical_and(row == level, lane == 2)
        means_ref[level] = jnp.sum(jnp.where(here, level_means, 0.0))
        maxima_ref[level] = jnp.sum(jnp.where(here, largest, 0.0))


def per_device(row_devices, col_devices, surface_field, land_words):
    rows, cols = surface_field.shape
    f32 = jnp.float32
    levels = tuple(
        jax.ShapeDtypeStruct((rows >> level, cols >> level), f32) for level in range(1, LEVELS + 1)
    )
    scratch = [
        pltpu.VMEM((cols // LANES, rows, LANES), f32),
        pltpu.VMEM((rows + 2 * HALO, LANES), jnp.int32),
        pltpu.VMEM((rows + 2 * HALO, LANES), f32),
        pltpu.VMEM((2 * HALO, rows), f32),
        pltpu.VMEM((2 * HALO, rows), f32),
        pltpu.VMEM((2 * HALO, rows + 2 * LANES), f32),
        pltpu.VMEM((2 * HALO, rows + 2 * LANES), f32),
        pltpu.VMEM((HALO, cols), f32),
        pltpu.VMEM((HALO, cols), f32),
        pltpu.VMEM((land_words.shape[1], LANES), jnp.int32),
        pltpu.VMEM((land_words.shape[1], LANES), jnp.int32),
    ]
    for level in range(LEVELS):
        shape = ((cols >> level) // LANES + 2, (rows >> level) + 48, LANES)
        scratch += [pltpu.VMEM(shape, f32)] * 2
    others = row_devices + col_devices - 2
    scratch += [
        pltpu.VMEM((4 * (rows // 2 + 16), cols + 2 * LANES), jnp.bfloat16),
        pltpu.VMEM((8, LANES), f32),
        pltpu.VMEM((8, LANES), f32),
        pltpu.VMEM((others, 8, LANES), f32),
        pltpu.SemaphoreType.DMA((cols // LANES,)),
        pltpu.SemaphoreType.DMA((10,)),
        pltpu.SemaphoreType.DMA((10,)),
        pltpu.SemaphoreType.DMA((others,)),
        pltpu.SemaphoreType.DMA((others,)),
    ]
    vmem = pl.BlockSpec(memory_space=pltpu.VMEM)
    smem = pl.BlockSpec(memory_space=pltpu.SMEM)
    small = jax.ShapeDtypeStruct((LEVELS,), f32)
    found = pl.pallas_call(
        functools.partial(kernel, row_devices, col_devices),
        out_shape=(*levels, small, small),
        in_specs=[pl.BlockSpec(memory_space=pl.ANY), vmem],
        out_specs=(vmem, vmem, vmem, vmem, smem, smem),
        scratch_shapes=scratch,
        compiler_params=pltpu.CompilerParams(
            collective_id=0, has_side_effects=True, vmem_limit_bytes=60 * 1024 * 1024
        ),
        name="coarsen_levels",
    )(surface_field, land_words.T)

    any_place = pl.BlockSpec(memory_space=pl.ANY)
    return pl.pallas_call(
        hand_over,
        out_shape=(*levels, small, small),
        in_specs=[vmem] * LEVELS + [smem] * 2,
        out_specs=(any_place,) * LEVELS + (smem,) * 2,
        scratch_shapes=[pltpu.SemaphoreType.DMA((LEVELS,))],
        name="hand_over",
    )(*found)


def hand_over(*refs):
    count = LEVELS + 2
    sources, targets, sems = refs[:count], refs[count : 2 * count], refs[2 * count]
    copies = [
        pltpu.make_async_copy(sources[at], targets[at], sems.at[at]) for at in range(LEVELS)
    ]
    for copy in copies:
        copy.start()
    for at in range(LEVELS):
        targets[LEVELS][at] = sources[LEVELS][at]
        targets[LEVELS + 1][at] = sources[LEVELS + 1][at]
    for copy in copies:
        copy.wait()


def solution(mesh):
    return jax.shard_map(
        functools.partial(per_device, mesh.shape["rows"], mesh.shape["cols"]),
        mesh=mesh,
        in_specs=(P("rows", "cols"), P("rows", "cols")),
        out_specs=(
            P("rows", "cols"),
            P("rows", "cols"),
            P("rows", "cols"),
            P("rows", "cols"),
            P(),
            P(),
        ),
        check_vma=False,
    )
```

```python
import functools
import math

import jax
import jax.numpy as jnp
from jax import lax
from jax.experimental import pallas as pl
from jax.experimental.pallas import tpu as pltpu
from jax.sharding import PartitionSpec as P

stencil_weights = (0.125, 0.375, 0.375, 0.125)
floor_value = 0.05
mean_eps = 1e-06
LEVELS = 4
LANES = 128
HALO = 16
MESH = pl.DeviceIdType.MESH


def kernel(
    row_devices,
    col_devices,
    field,
    land,
    level_one,
    level_two,
    level_three,
    level_four,
    means_ref,
    maxima_ref,
    fine,
    words,
    cosines,
    send_left,
    send_right,
    from_left,
    from_right,
    rows_top,
    rows_bottom,
    land_top,
    land_bottom,
    p0,
    c0,
    p1,
    c1,
    p2,
    c2,
    p3,
    c3,
    split,
    stat_own,
    stat_all,
    load_sem,
    halo_send,
    halo_recv,
    stat_send,
    stat_recv,
):
    rows, cols = field.shape
    tiles = cols // LANES
    count_words = land.shape[0]
    row_at = lax.axis_index("rows")
    col_at = lax.axis_index("cols")
    total_rows = rows * row_devices

    def device(down, right):
        return (
            lax.rem(row_at + down + row_devices, row_devices),
            lax.rem(col_at + right + col_devices, col_devices),
        )

    others = [
        (down, right)
        for down in range(row_devices)
        for right in range(col_devices)
        if (down, right) != (0, 0)
    ]

    def load(tile):
        start = tile * LANES
        if not isinstance(tile, int):
            start = pl.multiple_of(start, LANES)
        return pltpu.make_async_copy(
            field.at[:, pl.ds(start, LANES)], fine.at[tile], load_sem.at[tile]
        )

    load(0).start()
    load(tiles - 1).start()
    for tile in range(1, tiles - 1):
        load(tile).start()

    barrier = pltpu.get_barrier_semaphore()
    for down, right in others:
        pl.semaphore_signal(barrier, inc=1, device_id=device(down, right), device_id_type=MESH)

    def upright(array):
        if count_words < LANES:
            filler = jnp.zeros((LANES - count_words, array.shape[1]), jnp.int32)
            array = jnp.concatenate([array, filler], axis=0)
        return jnp.transpose(array)

    words[HALO : HALO + rows, :] = upright(land[...])
    lane = lax.broadcasted_iota(jnp.int32, (8, LANES), 1)

    def flags(tile, start, count):
        lanes = lax.broadcasted_iota(jnp.int32, (count, LANES), 1)
        place = tile * (LANES // 32) + lax.shift_right_logical(lanes, 5)
        word = jnp.take_along_axis(
            words[pl.ds(start, count), :], place, axis=1, mode="promise_in_bounds"
        )
        return jnp.bitwise_and(
            lax.shift_right_logical(word, jnp.bitwise_and(lanes, 31)), 1
        ).astype(jnp.float32)

    blocks = -(-(rows + 2 * HALO) // LANES)
    packed = (8 * (-(-blocks // 8)), LANES)
    row_index = (
        row_at * rows
        - HALO
        + lax.broadcasted_iota(jnp.int32, packed, 0) * LANES
        + lax.broadcasted_iota(jnp.int32, packed, 1)
    )
    latitude = ((row_index.astype(jnp.float32) + 0.5) / total_rows - 0.5) * math.pi
    on_globe = jnp.logical_and(row_index >= 0, row_index < total_rows)
    packed_cosines = jnp.where(on_globe, jnp.cos(latitude), 0.0)
    for block in range(blocks):
        size = min(LANES, rows + 2 * HALO - block * LANES)
        spread = jnp.broadcast_to(packed_cosines[block : block + 1, :], (LANES, LANES))
        cosines[block * LANES : block * LANES + size, :] = jnp.transpose(spread)[0:size, :]

    load(0).wait()
    send_left[0:HALO, :] = jnp.transpose(fine[0])[0:HALO, :]
    send_left[HALO:, :] = jnp.transpose(flags(0, HALO, rows))[0:HALO, :]
    load(tiles - 1).wait()
    send_right[0:HALO, :] = jnp.transpose(fine[tiles - 1])[LANES - HALO :, :]
    send_right[HALO:, :] = jnp.transpose(flags(tiles - 1, HALO, rows))[LANES - HALO :, :]

    zero_pad = ((p0, c0, 8), (p1, c1, 16), (p2, c2, 16), (p3, c3, 16))
    for product, cover, width in zero_pad:
        for ref in (product, cover):
            shape = (ref.shape[0], width, LANES)
            ref[:, 0:width, :] = jnp.zeros(shape, jnp.float32)
            ref[:, ref.shape[1] - width :, :] = jnp.zeros(shape, jnp.float32)

    pl.semaphore_wait(barrier, len(others))
    plan = (
        (field.at[rows - HALO : rows, :], rows_top, (1, 0)),
        (field.at[0:HALO, :], rows_bottom, (-1, 0)),
        (land.at[:, rows - LANES : rows], land_top, (1, 0)),
        (land.at[:, 0:LANES], land_bottom, (-1, 0)),
        (send_left, from_right.at[:, LANES : LANES + rows], (0, -1)),
        (send_right, from_left.at[:, LANES : LANES + rows], (0, 1)),
        (send_left.at[:, 0:LANES], from_right.at[:, LANES + rows :], (-1, -1)),
        (send_right.at[:, 0:LANES], from_left.at[:, LANES + rows :], (-1, 1)),
        (send_left.at[:, rows - LANES :], from_right.at[:, 0:LANES], (1, -1)),
        (send_right.at[:, rows - LANES :], from_left.at[:, 0:LANES], (1, 1)),
    )
    copies = []
    for place, (source, target, (down, right)) in enumerate(plan):
        copy = pltpu.make_async_remote_copy(
            src_ref=source,
            dst_ref=target,
            send_sem=halo_send.at[place],
            recv_sem=halo_recv.at[place],
            device_id=device(down, right),
            device_id_type=MESH,
        )
        copy.start()
        copies.append(copy)

    def own_tile(tile):
        for start in range(0, rows, 64):
            cover = flags(tile, HALO + start, 64) * cosines[HALO + start : HALO + start + 64, :]
            c0[tile + 1, 24 + start : 88 + start, :] = cover
            p0[tile + 1, 24 + start : 88 + start, :] = cover * fine[tile, start : start + 64, :]

    own_tile(0)
    own_tile(tiles - 1)

    @pl.loop(1, tiles - 1)
    def _(tile):
        load(tile).wait()
        own_tile(tile)

    for copy in copies:
        copy.wait()

    words[0:HALO, :] = upright(land_top[...])[LANES - HALO :, :]
    words[HALO + rows :, :] = upright(land_bottom[...])[0:HALO, :]
    for landed, at in ((rows_top, 0), (rows_bottom, HALO + rows)):
        for tile in range(tiles):
            cover = flags(tile, at, HALO) * cosines[at : at + HALO, :]
            c0[tile + 1, 8 + at : 8 + at + HALO, :] = cover
            p0[tile + 1, 8 + at : 8 + at + HALO, :] = (
                cover * landed[:, tile * LANES : (tile + 1) * LANES]
            )
    filler = jnp.zeros((LANES - HALO, rows + 2 * LANES), jnp.float32)
    first = LANES - HALO
    last = LANES + rows + HALO
    for packet, tile, at_end in ((from_left, 0, True), (from_right, tiles + 1, False)):
        sides = []
        for part in (packet[0:HALO, :], packet[HALO:, :]):
            pieces = [filler, part] if at_end else [part, filler]
            sides.append(jnp.transpose(jnp.concatenate(pieces, axis=0))[first:last, :])
        cover = sides[1] * cosines[...]
        c0[tile, 8 : 8 + rows + 2 * HALO, :] = cover
        p0[tile, 8 : 8 + rows + 2 * HALO, :] = cover * sides[0]

    band_row = lax.broadcasted_iota(jnp.int32, (4 * LANES, LANES), 0)
    band_col = lax.broadcasted_iota(jnp.int32, (4 * LANES, LANES), 1)
    tap = band_row - (LANES - 1) - 2 * band_col
    band = jnp.where(
        jnp.logical_or(tap == 0, tap == 3),
        stencil_weights[0],
        jnp.where(jnp.logical_or(tap == 1, tap == 2), stencil_weights[1], 0.0),
    ).astype(jnp.bfloat16)

    stats = []
    sources = ((p0, c0), (p1, c1), (p2, c2), (p3, c3))
    outputs = (level_one, level_two, level_three, level_four)
    for level in range(LEVELS):
        product_in, cover_in = sources[level]
        output = outputs[level]
        own = output.shape[0]
        count = own + 16
        tiles_in = product_in.shape[0]
        tiles_out = output.shape[1] // LANES

        @pl.loop(0, tiles_in)
        def _(tile):
            offset = pl.multiple_of(tile * LANES, LANES)
            for place, ref in enumerate((product_in, cover_in)):
                taps = [ref[tile, pl.ds(7 + a, count, stride=2), :] for a in range(4)]
                down = stencil_weights[0] * (taps[0] + taps[3]) + stencil_weights[1] * (
                    taps[1] + taps[2]
                )
                high = down.astype(jnp.bfloat16)
                low = (down - high.astype(jnp.float32)).astype(jnp.bfloat16)
                at = 2 * place * count
                split[at : at + count, pl.ds(offset, LANES)] = high
                split[at + count : at + 2 * count, pl.ds(offset, LANES)] = low

        index = row_at * own - 8 + lax.broadcasted_iota(jnp.int32, (count, LANES), 0)
        inside = jnp.logical_and(index >= 0, index < own * row_devices)

        def across(start, width, table):
            result = jnp.dot(
                split[0 : 4 * count, pl.ds(start, width)],
                table,
                preferred_element_type=jnp.float32,
            )
            num = result[0:count] + result[count : 2 * count]
            den = result[2 * count : 3 * count] + result[3 * count :]
            value = num / jnp.maximum(den, floor_value)
            cover = jnp.where(inside, den, 0.0)
            return value, cover, cover * value

        def keep(tile, cover, product):
            if level + 1 < LEVELS:
                product_out, cover_out = sources[level + 1]
                product_out[tile, 16 : 16 + count, :] = product
                cover_out[tile, 16 : 16 + count, :] = cover

        if level + 1 < LEVELS:
            value, cover, product = across(0, 2 * LANES, band[2 * LANES :])
            keep(0, cover, product)
            value, cover, product = across((tiles_in - 2) * LANES, 2 * LANES, band[: 2 * LANES])
            keep(tiles_out + 1, cover, product)

        def own_columns(tile, carry):
            weighted, total, largest = carry
            value, cover, product = across(
                pl.multiple_of(tile * 2 * LANES, 2 * LANES), 4 * LANES, band
            )
            keep(tile + 1, cover, product)
            output[:, pl.ds(pl.multiple_of(tile * LANES, LANES), LANES)] = value[8 : 8 + own]

            def parts(array):
                return array[8 : 8 + own].reshape(own // 8, 8, LANES)

            return (
                weighted + jnp.sum(parts(product), axis=0),
                total + jnp.sum(parts(cover), axis=0),
                jnp.maximum(largest, jnp.max(parts(value), axis=0)),
            )

        zero = jnp.zeros((8, LANES), jnp.float32)
        start = (zero, zero, jnp.full((8, LANES), -jnp.inf, jnp.float32))
        stats.append(lax.fori_loop(0, tiles_out, own_columns, start))

    row = lax.broadcasted_iota(jnp.int32, (8, LANES), 0)
    gathered = []
    for kind, reduce in ((0, jnp.sum), (1, jnp.sum), (2, jnp.max)):
        tile = jnp.zeros((8, LANES), jnp.float32)
        for level in range(LEVELS):
            tile = jnp.where(row == level, reduce(stats[level][kind], axis=0, keepdims=True), tile)
        gathered.append(reduce(tile, axis=1, keepdims=True))
    stat_own[...] = jnp.where(
        lane == 0, gathered[0], jnp.where(lane == 1, gathered[1], gathered[2])
    )
    copies = []
    for place, (down, right) in enumerate(others):
        copy = pltpu.make_async_remote_copy(
            src_ref=stat_own,
            dst_ref=stat_all.at[place],
            send_sem=stat_send.at[place],
            recv_sem=stat_recv.at[place],
            device_id=device(down, right),
            device_id_type=MESH,
        )
        copy.start()
        copies.append(copy)
    for copy in copies:
        copy.wait()
    summed = stat_own[...] + jnp.sum(stat_all[...], axis=0)
    largest = jnp.maximum(stat_own[...], jnp.max(stat_all[...], axis=0))
    weighted = jnp.sum(jnp.where(lane == 0, summed, 0.0), axis=1, keepdims=True)
    total = jnp.sum(jnp.where(lane == 1, summed, 0.0), axis=1, keepdims=True)
    level_means = jnp.broadcast_to(weighted / (total + mean_eps), (8, LANES))
    for level in range(LEVELS):
        here = jnp.logical_and(row == level, lane == 2)
        means_ref[level] = jnp.sum(jnp.where(here, level_means, 0.0))
        maxima_ref[level] = jnp.sum(jnp.where(here, largest, 0.0))


def per_device(row_devices, col_devices, surface_field, land_words):
    rows, cols = surface_field.shape
    f32 = jnp.float32
    levels = tuple(
        jax.ShapeDtypeStruct((rows >> level, cols >> level), f32) for level in range(1, LEVELS + 1)
    )
    scratch = [
        pltpu.VMEM((cols // LANES, rows, LANES), f32),
        pltpu.VMEM((rows + 2 * HALO, LANES), jnp.int32),
        pltpu.VMEM((rows + 2 * HALO, LANES), f32),
        pltpu.VMEM((2 * HALO, rows), f32),
        pltpu.VMEM((2 * HALO, rows), f32),
        pltpu.VMEM((2 * HALO, rows + 2 * LANES), f32),
        pltpu.VMEM((2 * HALO, rows + 2 * LANES), f32),
        pltpu.VMEM((HALO, cols), f32),
        pltpu.VMEM((HALO, cols), f32),
        pltpu.VMEM((land_words.shape[1], LANES), jnp.int32),
        pltpu.VMEM((land_words.shape[1], LANES), jnp.int32),
    ]
    for level in range(LEVELS):
        shape = ((cols >> level) // LANES + 2, (rows >> level) + 48, LANES)
        scratch += [pltpu.VMEM(shape, f32)] * 2
    others = row_devices * col_devices - 1
    scratch += [
        pltpu.VMEM((4 * (rows // 2 + 16), cols + 2 * LANES), jnp.bfloat16),
        pltpu.VMEM((8, LANES), f32),
        pltpu.VMEM((others, 8, LANES), f32),
        pltpu.SemaphoreType.DMA((cols // LANES,)),
        pltpu.SemaphoreType.DMA((10,)),
        pltpu.SemaphoreType.DMA((10,)),
        pltpu.SemaphoreType.DMA((others,)),
        pltpu.SemaphoreType.DMA((others,)),
    ]
    vmem = pl.BlockSpec(memory_space=pltpu.VMEM)
    smem = pl.BlockSpec(memory_space=pltpu.SMEM)
    small = jax.ShapeDtypeStruct((LEVELS,), f32)
    found = pl.pallas_call(
        functools.partial(kernel, row_devices, col_devices),
        out_shape=(*levels, small, small),
        in_specs=[pl.BlockSpec(memory_space=pl.ANY), vmem],
        out_specs=(vmem, vmem, vmem, vmem, smem, smem),
        scratch_shapes=scratch,
        compiler_params=pltpu.CompilerParams(
            collective_id=0, has_side_effects=True, vmem_limit_bytes=60 * 1024 * 1024
        ),
        name="coarsen_levels",
    )(surface_field, land_words.T)

    any_place = pl.BlockSpec(memory_space=pl.ANY)
    return pl.pallas_call(
        hand_over,
        out_shape=(*levels, small, small),
        in_specs=[vmem] * LEVELS + [smem] * 2,
        out_specs=(any_place,) * LEVELS + (smem,) * 2,
        scratch_shapes=[pltpu.SemaphoreType.DMA((LEVELS,))],
        name="hand_over",
    )(*found)


def hand_over(*refs):
    count = LEVELS + 2
    sources, targets, sems = refs[:count], refs[count : 2 * count], refs[2 * count]
    copies = [
        pltpu.make_async_copy(sources[at], targets[at], sems.at[at]) for at in range(LEVELS)
    ]
    for copy in copies:
        copy.start()
    for at in range(LEVELS):
        targets[LEVELS][at] = sources[LEVELS][at]
        targets[LEVELS + 1][at] = sources[LEVELS + 1][at]
    for copy in copies:
        copy.wait()


def solution(mesh):
    return jax.shard_map(
        functools.partial(per_device, mesh.shape["rows"], mesh.shape["cols"]),
        mesh=mesh,
        in_specs=(P("rows", "cols"), P("rows", "cols")),
        out_specs=(
            P("rows", "cols"),
            P("rows", "cols"),
            P("rows", "cols"),
            P("rows", "cols"),
            P(),
            P(),
        ),
        check_vma=False,
    )
```
